32 devices in a mesh: expert: 8 (over y, x, core), dp: 4 (over z).
Axes of the slice: x: 2, y: 2, z: 4, core: 2. Of those that a mesh axis runs over, the one named last changes fastest.
Arguments:
- tokens: bfloat16 [256, 4096], P(('expert', 'dp')), may hold values from -6 to 6
- expert_ids: int32 [256, 2], P(('expert', 'dp')), may hold values from 0 to 7, all different within a row; in each aligned block of 8 rows (0 to 7, 8 to 15, ...) at most 4 rows name the same one
- gate_q: int32 [256, 2], P(('expert', 'dp')), may hold values from 1 to 255
- capacity: int32 [8], replicated, may hold values from 2 to 4, as said below
- w_gate: bfloat16 [8, 4096, 14336], P('dp', None, 'expert'), may hold values from -0.09375 to 0.09375
- w_up: bfloat16 [8, 4096, 14336], P('dp', None, 'expert'), may hold values from -0.09375 to 0.09375
- w_down: bfloat16 [8, 14336, 4096], P('dp', 'expert'), may hold values from -0.046875 to 0.046875
Outputs:
- mixed: bfloat16 [256, 4096], P(('expert', 'dp'))
The draws below stay inside these ranges and needn't reach their ends.
Inputs may be any that keep to these rules, and one draw needn't show every extreme that they name: `expert_ids`: each token names two different experts; among the tokens of one device no expert is named more than 4 times. `capacity`: at least half of the experts have exactly 4.
All inputs are finite; a program needn't handle non-finite values.
Results may differ from the reference program's by a relative error of at most 0.005.
Values may be sent and summed in bfloat16 or wider, within the bound.
No kernel may reach another device: no remote copies, remote signals or barrier semaphores. Data moves between devices by JAX's collectives and lax.ppermute only.
A program may use at most 192 MiB of HBM per device.

```python
import math
import jax
import jax.numpy as jnp
import numpy as np
from jax import lax

D = 4096
FF = 14336
EXPERTS = 8
TOK_DEV = 8
CAP = 4
TOKENS = 256


def draw_capacity(key, part):
    folded = jax.random.fold_in(key, 11)
    low_key, pick_key = jax.random.split(folded)
    lowered = jax.random.randint(low_key, (EXPERTS,), 2, CAP + 1)
    order = jax.random.permutation(pick_key, EXPERTS)
    return jnp.where(order < EXPERTS // 2, CAP, lowered).astype(jnp.int32)


def touch_ends(values, stream_key, least, top_value):
    shape = values.shape
    place = [jax.random.randint(jax.random.fold_in(stream_key, axis), (), 0, shape[axis]) for axis in range(len(shape))]
    values = values.at[tuple(place)].set(least)
    longest = shape.index(max(shape))
    place[longest] = (place[longest] + 1) % shape[longest]
    return values.at[tuple(place)].set(top_value)


def block_scale(stream_key, extent, cuts, smallest, high):
    loudness = 1.0
    for position, parts in cuts:
        heights = jax.random.uniform(jax.random.fold_in(jax.random.fold_in(stream_key, 6), position), (parts,), jnp.float32, smallest / len(cuts), high / len(cuts))
        loudness = loudness * jnp.repeat(jnp.exp(heights), extent[position] // parts).reshape((-1,) + (1,) * (len(extent) - 1 - position))
    return loudness


def deal_out(key, own, number, rows, amount, top, most, slope):
    sequence = jax.random.permutation(key, amount)
    crowded, usual = load_shares(amount, rows * top, most, slope, True), load_shares(amount, rows * top, most, slope, False)
    places = jnp.arange(amount)

    def named(sizes, offset_by):
        used = int((sizes > 0).sum())
        fixed = max(1, used // 4)
        passed = fixed + (places - fixed + offset_by * (used - fixed)) % max(1, amount - fixed)
        return jnp.zeros((amount,), jnp.int32).at[sequence[jnp.where(places < fixed, places, passed)]].set(jnp.asarray(sizes, jnp.int32))

    sizes = jnp.where(number % 4 == 0, named(crowded, number // 4), named(usual, number - number // 4 - 1))
    mixed = jax.random.permutation(jax.random.fold_in(own, 3), amount)
    giver, receiver = mixed[0:amount // 2 * 2:2], mixed[1:amount // 2 * 2:2]
    slack = jnp.minimum(sizes[giver] - 1, most - sizes[receiver]) // 2
    slack = jnp.where((giver == sequence[0]) | (receiver == sequence[0]) | (sizes[receiver] == 0), 0, jnp.maximum(slack, 0))
    passed = jax.random.randint(jax.random.fold_in(own, 4), (amount // 2,), 0, 1 << 20) % (slack + 1)
    sizes = sizes.at[giver].add(-passed).at[receiver].add(passed)
    labels = jnp.searchsorted(jnp.cumsum(sizes), jnp.arange(rows * top), side="right").astype(jnp.int32)
    listing = labels.reshape(top, rows).T
    listing = listing[jax.random.permutation(jax.random.fold_in(own, 1), rows)]
    offset_by = jax.random.randint(jax.random.fold_in(own, 2), (rows, 1), 0, top)
    return jnp.take_along_axis(listing, (jnp.arange(top)[None, :] + offset_by) % top, axis=1)


def load_shares(amount, total, limit, slope, full):
    weights = [(1 << 20) // math.isqrt(grade ** slope) + 1 for grade in range(1, amount + 1)]
    largest = limit if full else min(limit, max(-(-total // amount), total * weights[0] // sum(weights)))
    least = 1 if total - largest >= amount - 1 else 0
    counts, spare = [largest] + [least] * (amount - 1), total - largest - least * (amount - 1)
    while spare > 0:
        candidates = [i for i in range(1, amount) if counts[i] < largest] or [i for i in range(1, amount) if counts[i] < limit]
        whole, left = sum([weights[i] for i in candidates]), spare
        for i in candidates:
            more = min(limit - counts[i], max(1, left * weights[i] // whole), spare)
            counts[i] = counts[i] + more
            spare = spare - more
    return np.array(counts)


def scatter_about(rng, extent, scale, bound, cuts=(), kind=jnp.bfloat16):
    drawn = jax.random.normal(rng, extent, jnp.float32) * scale
    if len(cuts) > 0:
        drawn = block_scale(rng, extent, cuts, -0.22, 0.18) * drawn
    return jnp.clip(drawn, min=-bound, max=bound).astype(kind)


def setup_inputs(seed: int = 0) -> dict:
    seeds = jax.random.split(jax.random.key(seed), 8)
    tokens = scatter_about(seeds[0], (TOKENS, D), 1.0, 6.0, ((0, 32),))
    expert_ids_keys = jax.random.split(jax.random.fold_in(seeds[1], 1), TOKENS // TOK_DEV)
    expert_ids_turns = jax.random.permutation(jax.random.fold_in(seeds[1], 3), TOKENS // TOK_DEV)
    expert_ids = jax.vmap(lambda own, number: deal_out(jax.random.fold_in(seeds[1], 2), own, number, TOK_DEV, EXPERTS, 2, CAP, 2))(expert_ids_keys, expert_ids_turns).reshape((TOKENS, 2))
    gate_q = touch_ends(jax.random.randint(seeds[2], (TOKENS, 2), 1, 256), jax.random.fold_in(seeds[2], 1), 1, 255).astype(jnp.int32)
    capacity = draw_capacity(jax.random.fold_in(seeds[7], 71), 0)
    w_gate = scatter_about(seeds[4], (EXPERTS, D, FF), D ** -0.5, 0.09375, ((0, 4), (2, 8)))
    w_up = scatter_about(seeds[5], (EXPERTS, D, FF), D ** -0.5, 0.09375, ((0, 4), (2, 8)))
    w_down = scatter_about(seeds[6], (EXPERTS, FF, D), FF ** -0.5, 0.046875, ((0, 4), (1, 8)))
    return dict(tokens=tokens, expert_ids=expert_ids, gate_q=gate_q, capacity=capacity, w_gate=w_gate, w_up=w_up, w_down=w_down)


def slot_table(expert_ids, capacity):
    flat_ids = expert_ids.reshape(-1)
    matches = (flat_ids[:, None] == jnp.arange(EXPERTS, dtype=jnp.int32)[None, :]).astype(jnp.int32)
    before = jnp.cumsum(matches, axis=0) - matches
    rank_in = jnp.sum(before * matches, axis=1)
    limit_of = jnp.sum(matches * capacity[None, :], axis=1)
    slot_of = flat_ids * CAP + rank_in
    chosen = slot_of[None, :] == jnp.arange(EXPERTS * CAP, dtype=jnp.int32)[:, None]
    return chosen & (rank_in < limit_of)[None, :]


def mixing(gate_q):
    levels = gate_q.astype(jnp.float32)
    return (levels / jnp.sum(levels, axis=1, keepdims=True)).reshape(-1)


def expert_block(operands):
    slot_rows, gate_mat, up_mat, down_mat = operands
    gate_val = jnp.dot(slot_rows, gate_mat, preferred_element_type=jnp.float32)
    up_value = jnp.dot(slot_rows, up_mat, preferred_element_type=jnp.float32)
    hidden = (jax.nn.silu(gate_val) * up_value).astype(jnp.bfloat16)
    return jnp.dot(hidden, down_mat, preferred_element_type=jnp.float32)


def reference(tokens, expert_ids, gate_q, capacity, w_gate, w_up, w_down):
    blocks = TOKENS // TOK_DEV
    token_blocks = tokens.reshape(blocks, TOK_DEV, D)
    tables = jax.vmap(slot_table, in_axes=(0, None))(expert_ids.reshape(blocks, TOK_DEV, 2), capacity)
    mixes = jax.vmap(mixing)(gate_q.reshape(blocks, TOK_DEV, 2))
    picker = tables.reshape(blocks, EXPERTS * CAP, TOK_DEV, 2).sum(axis=3).astype(jnp.float32)
    slot_rows = jnp.einsum("bst,btd->bsd", picker, token_blocks.astype(jnp.float32),
                           precision=lax.Precision.HIGHEST).astype(jnp.bfloat16)
    per_expert = slot_rows.reshape(blocks, EXPERTS, CAP, D).transpose(1, 0, 2, 3).reshape(EXPERTS, blocks * CAP, D)
    outputs = lax.map(expert_block, (per_expert, w_gate, w_up, w_down))
    outputs = outputs.reshape(EXPERTS, blocks, CAP, D).transpose(1, 0, 2, 3).reshape(blocks, EXPERTS * CAP, D)
    combine = tables.astype(jnp.float32) * mixes[:, None, :]
    spread = jnp.einsum("bsa,bsd->bad", combine, outputs, precision=lax.Precision.HIGHEST)
    mixed = spread.reshape(blocks, TOK_DEV, 2, D).sum(axis=2)
    return mixed.reshape(TOKENS, D).astype(jnp.bfloat16)
```

```python
import jax
import jax.numpy as jnp
from jax import lax
from jax.experimental import pallas as pl
from jax.experimental.pallas import tpu as pltpu
from jax.sharding import PartitionSpec as P


CAP = 4
LANES = 128
MIB = 1 << 20


VMEM = pl.BlockSpec(memory_space=pltpu.VMEM)
ANY = pl.BlockSpec(memory_space=pl.ANY)
HBM = pl.BlockSpec(memory_space=pltpu.HBM)
SMEM = pl.BlockSpec(memory_space=pltpu.SMEM)


def params(mib):
    return pltpu.CompilerParams(vmem_limit_bytes=int(mib * MIB))


def in_hbm(array):
    return pltpu.with_memory_space_constraint(array, pltpu.HBM)


def iota(shape, dim):
    return lax.broadcasted_iota(jnp.int32, shape, dim)


def pack(tokens, ids, levels, capacity, place):
    rows, width = tokens.shape
    experts = capacity.shape[0]

    def body(place_ref, ids_hbm, level_hbm, cap_hbm, tok_hbm, out_ref, info_ref, ids_ref, level_ref, cap_ref, sems):
        copies = [
            pltpu.make_async_copy(src, dst, sems.at[i])
            for i, (src, dst) in enumerate(
                (
                    (ids_hbm, ids_ref),
                    (level_hbm, level_ref),
                    (cap_hbm, cap_ref),
                    (tok_hbm, out_ref.at[:, pl.ds(0, width)]),
                )
            )
        ]
        for copy in copies:
            copy.start()
        for copy in copies:
            copy.wait()
        eye = iota((rows, rows), 0) == iota((rows, rows), 1)
        lower = (iota((rows, rows), 1) < iota((rows, rows), 0)).astype(jnp.float32)
        expert = iota((rows, experts), 1).astype(jnp.float32)
        limits = cap_ref[...].astype(jnp.float32)

        def column(ref, k):
            return jnp.sum(jnp.where(eye, ref[k : k + 1, :].astype(jnp.float32), 0.0), axis=1, keepdims=True)

        named = [column(ids_ref, k) for k in range(2)]
        hot = [(expert == col).astype(jnp.float32) for col in named]
        before = jnp.dot(lower, hot[0] + hot[1], preferred_element_type=jnp.float32)
        level = [column(level_ref, k) for k in range(2)]
        total = level[0] + level[1]
        lane = iota((rows, LANES), 1)
        slots = jnp.full((rows, LANES), -1.0, jnp.float32)
        info = slots
        for k in range(2):
            rank = jnp.sum(hot[k] * before, axis=1, keepdims=True)
            limit = jnp.sum(hot[k] * limits, axis=1, keepdims=True)
            slot = jnp.where(rank < limit, named[k] * CAP + rank, -1.0)
            slots = jnp.where(lane == k, slot, slots)
            info = jnp.where(lane == k, slot, jnp.where(lane == 2 + k, level[k] / total, info))
        for i in range(2):
            info = jnp.where(lane == 4 + i, place_ref[i].astype(jnp.float32), info)
        out_ref[:, width:] = slots.astype(jnp.bfloat16)
        info_ref[...] = info

    return pl.pallas_call(
        body,
        in_specs=[SMEM] + [HBM] * 4,
        out_specs=[VMEM] * 2,
        out_shape=[
            jax.ShapeDtypeStruct((rows, width + LANES), jnp.bfloat16),
            jax.ShapeDtypeStruct((rows, LANES), jnp.float32),
        ],
        scratch_shapes=[
            pltpu.VMEM(ids.shape, jnp.int32),
            pltpu.VMEM(levels.shape, jnp.int32),
            pltpu.VMEM((1, experts), jnp.int32),
            pltpu.SemaphoreType.DMA((4,)),
        ],
        compiler_params=params(0.5),
        name="pack",
    )(place, *map(in_hbm, (ids, levels, capacity.reshape(1, experts), tokens)))


def mix_back(info, pieces, local):
    rows = info.shape[0]
    width = pieces[0].shape[1]
    span = local * CAP

    def body(info_ref, *refs):
        *ins, out_ref = refs
        here = info_ref[:, 4:5].astype(jnp.int32)
        row = iota((rows, span), 1)
        weights = []
        for q in range(len(ins)):
            group = here ^ q
            weight = jnp.zeros((rows, span), jnp.float32)
            for k in range(2):
                slot = info_ref[:, k : k + 1].astype(jnp.int32) - group * span
                if q % 2:
                    slot = jnp.where((slot < 0) | (slot >= span), -1, slot ^ CAP)
                weight = weight + jnp.where(row == slot, info_ref[:, 2 + k : 3 + k], 0.0)
            weights.append(weight)
        weight = jnp.concatenate(weights, axis=1)
        terms = []
        for _ in range(3):
            terms.append(weight.astype(jnp.bfloat16).astype(jnp.float32))
            weight = weight - terms[-1]
        terms = jnp.concatenate(terms + [jnp.zeros_like(weight)], axis=0).astype(jnp.bfloat16)
        blocks = jnp.concatenate([ref[...] for ref in ins], axis=0)
        sums = jnp.dot(terms, blocks, preferred_element_type=jnp.float32)
        total = sums[:rows] + sums[rows : 2 * rows] + sums[2 * rows : 3 * rows]
        out_ref[...] = total.astype(jnp.bfloat16)

    return pl.pallas_call(
        body,
        in_specs=[VMEM] * (1 + len(pieces)),
        out_specs=VMEM,
        out_shape=jax.ShapeDtypeStruct((rows, width), jnp.bfloat16),
        compiler_params=params(8),
        name="mix_back",
    )(info, *pieces)


def fetch(weights, member, splits, after):
    depth = weights.shape[1]
    parts = 4
    step = depth // parts
    count = len(splits)

    def body(w_ref, after_ref, *refs):
        outs, done_ref, sems = refs[:count], refs[count], refs[count + 1]
        copies = []
        for j, (first, width) in enumerate(splits):
            for i in range(parts):
                part = pl.ds(i * step, step)
                copies.append(
                    pltpu.make_async_copy(
                        w_ref.at[member, part, pl.ds(first, width)], outs[j].at[part], sems.at[j * parts + i]
                    )
                )
        for copy in copies:
            copy.start()
        for copy in copies:
            copy.wait()
        done_ref[...] = jnp.zeros_like(done_ref)

    *blocks, done = pl.pallas_call(
        body,
        in_specs=[HBM, ANY],
        out_specs=[VMEM] * (count + 1),
        out_shape=[pltpu.VMEM((depth, width), jnp.bfloat16) for _, width in splits]
        + [jax.ShapeDtypeStruct((8, LANES), jnp.float32)],
        scratch_shapes=[pltpu.SemaphoreType.DMA((parts * count,))],
        compiler_params=params(0.25),
    )(in_hbm(weights), after)
    return blocks, done


def joined(pieces, after):
    rows, width = pieces[0].shape
    count = len(pieces)

    def body(*refs):
        out_ref = refs[-1]
        for i in range(count):
            out_ref[i * rows : (i + 1) * rows, :] = refs[i][...]

    return pl.pallas_call(
        body,
        in_specs=[VMEM] * count + [ANY],
        out_specs=VMEM,
        out_shape=jax.ShapeDtypeStruct((count * rows, width), pieces[0].dtype),
        compiler_params=params(1),
    )(*pieces, after)


def picked(info, first, second, after):
    rows = first.shape[0]

    def body(info_ref, first_ref, second_ref, after_ref, out_ref):
        even = jnp.broadcast_to(info_ref[0:1, 5:6], (rows, 1)) == 0.0

        out_ref[...] = jnp.where(even, first_ref[...], second_ref[...])

    return pl.pallas_call(
        body,
        in_specs=[VMEM, VMEM, VMEM, ANY],
        out_specs=VMEM,
        out_shape=jax.ShapeDtypeStruct(first.shape, first.dtype),
        compiler_params=params(1),
    )(info, first, second, after)


def experts_kernel(pieces, info, held, tile, w_gate, w_up, w_down):
    local, width, units = w_gate.shape
    groups = len(pieces)
    piece_rows = pieces[0].shape[0]
    tokens = groups * piece_rows
    slots = tokens // 8 * CAP
    steps = units // tile
    down_steps = width // tile
    ring = 6
    batch = 2
    half = groups // 2 * piece_rows
    order = [(matrix, member) for member in range(local) for matrix in range(2)]
    given = [block for key in order for block in held[key]]

    def body(*refs):
        piece_refs = refs[:groups]
        info_ref = refs[groups]
        given_refs = list(refs[groups + 1 : groups + 1 + len(given)])
        wg, wu, wd, mine, theirs, toks, rows, hid, buf, sems = refs[groups + 1 + len(given) :]

        tiles, stream = {}, []
        for key in order:
            at = 0
            for block in held[key]:
                ref = given_refs.pop(0)
                for n in range(block.shape[1] // tile):
                    tiles[key, at] = (ref, n)
                    at += 1
        for member in range(local):
            for n in range(steps):
                for matrix in range(2):
                    if ((matrix, member), n) not in tiles:
                        tiles[(matrix, member), n] = len(stream)
                        stream.append(((wg, wu)[matrix], member, n))

        downs = len(stream)
        jobs = downs + down_steps

        def copies(i):
            at = i % ring
            if i < downs:
                w, member, n = stream[i]
                pairs = [(w.at[member, :, pl.ds(n * tile, tile)], buf.at[at])]
            else:
                cols = pl.ds((i - downs) * tile, tile)
                pairs = [(wd.at[m, :, cols], buf.at[at, pl.ds(m * units, units)]) for m in range(local)]
            return [pltpu.make_async_copy(*pair, sems.at[at, j]) for j, pair in enumerate(pairs)]

        def start(i):
            if i < jobs:
                for copy in copies(i):
                    copy.start()

        def wait(i):
            for copy in copies(i):
                copy.wait()

        for i in range(ring):
            start(i)

        first = info_ref[0:1, 4:5].astype(jnp.int32) * (local * CAP)
        token_block = iota((tokens, slots), 0) // 8
        slot = iota((tokens, slots), 1)
        slot_block = slot // CAP
        slot_rank = slot % CAP
        pick = [jnp.zeros((tokens, slots), jnp.bool_) for _ in range(local)]
        for g in range(groups):
            toks[g * piece_rows : (g + 1) * piece_rows, :] = piece_refs[g][:, :width]
        for k in range(2):
            code = jnp.concatenate(
                [ref[:, width : width + LANES].astype(jnp.float32)[:, k : k + 1] for ref in piece_refs], axis=0
            ).astype(jnp.int32)
            for m in range(local):
                hit = (code - first == slot_rank + m * CAP) & (token_block == (slot_block ^ m))
                pick[m] = pick[m] | hit
        pickers = [p.astype(jnp.float32).T.astype(jnp.bfloat16) for p in pick]

        def place(n, carry):
            cols = pl.ds(pl.multiple_of(n * tile, tile), tile)
            for m in range(local):
                rows[m, :, cols] = jnp.dot(pickers[m], toks[:, cols], preferred_element_type=jnp.float32).astype(
                    jnp.bfloat16
                )
            return carry

        lax.fori_loop(0, width // tile, place, 0)

        def product(matrix, m, n):
            spot = tiles[(matrix, m), n]
            if isinstance(spot, tuple):
                ref, at = spot
                block = ref[:, at * tile : (at + 1) * tile]
            else:
                block = buf[spot % ring, :width, :]
            return jnp.dot(rows[m], block, preferred_element_type=jnp.float32)

        def streamed(m, n):
            return [spot for matrix in range(2) if not isinstance(spot := tiles[(matrix, m), n], tuple)]

        waiting, ready = [], []
        for m in range(local):
            for n in range(steps):
                spots = streamed(m, n)
                if not spots:
                    ready.append(([(m, n)], []))
                elif waiting and len(waiting[-1][1]) + len(spots) <= batch:
                    waiting[-1][0].append((m, n))
                    waiting[-1][1].extend(spots)
                else:
                    waiting.append(([(m, n)], spots))
        turns = []
        while waiting or ready:
            turns += [queue.pop(0) for queue in (waiting, ready) if queue]
        for group, spots in turns:
            for spot in spots:
                wait(spot)
            for m, n in group:
                gate = product(0, m, n)
                up = product(1, m, n)
                act = gate * (1.0 / (1.0 + jnp.exp(-gate))) * up
                hid[m, :, n * tile : (n + 1) * tile] = act.astype(jnp.bfloat16)
            for spot in spots:
                start(spot + ring)

        low = iota((8, tile), 0) < CAP
        for n in range(down_steps):
            cols = slice(n * tile, (n + 1) * tile)
            if n % batch == 0:
                for i in range(n, min(n + batch, down_steps)):
                    wait(downs + i)
            slot_at = (downs + n) % ring
            outs = [
                jnp.dot(hid[m], buf[slot_at, m * units : (m + 1) * units, :], preferred_element_type=jnp.float32)
                for m in range(local)
            ]
            start(downs + n + ring)
            for j in range(slots // 8):
                a, b = (out[j * 8 : (j + 1) * 8] for out in outs)
                pair = jnp.concatenate([jnp.where(low, a, b), jnp.where(low, b, a)], axis=0)
                at = j * 16
                if at < half:
                    mine[at : at + 16, cols] = pair
                else:
                    theirs[at - half : at - half + 16, cols] = pair.astype(jnp.bfloat16)

    bf16 = jnp.bfloat16
    return pl.pallas_call(
        body,
        in_specs=[VMEM] * (groups + 1 + len(given)) + [HBM] * 3,
        out_specs=[VMEM] * 2,
        out_shape=[
            jax.ShapeDtypeStruct((half, width), jnp.float32),
            jax.ShapeDtypeStruct((half, width), bf16),
        ],
        scratch_shapes=[
            pltpu.VMEM((tokens, width), bf16),
            pltpu.VMEM((local, slots, width), bf16),
            pltpu.VMEM((local, slots, units), bf16),
            pltpu.VMEM((ring, max(width, local * units), tile), bf16),
            pltpu.SemaphoreType.DMA((ring, local)),
        ],
        compiler_params=params(18.2),
        name="experts",
    )(*pieces, info, *given, *map(in_hbm, (w_gate, w_up, w_down)))


def flip(size, bits):
    return [(i, i ^ bits) for i in range(size)]


def fast(tokens, expert_ids, gate_q, capacity, w_gate, w_up, w_down):
    size = lax.axis_size("expert")
    depth = lax.axis_size("dp")
    local, _, units = w_gate.shape
    core = jnp.bitwise_and(lax.axis_index("expert"), 1)
    place = jnp.stack([lax.axis_index("dp"), core]).astype(jnp.int32)
    mixed = [(i, i ^ (2 if i % 2 == 0 else 4)) for i in range(size)]

    packed, info = pack(tokens, expert_ids.T, gate_q.T, capacity, place)
    along = [packed] + [lax.ppermute(packed, "dp", flip(depth, k)) for k in range(1, depth)]
    tile = 256
    some, rest = 2 * tile, units - 4 * tile
    whole = ((0, some), (some, some), (2 * some, rest))
    gate0, gate0_done = fetch(w_gate, 0, whole, packed)
    base = joined(along, gate0_done)
    side_a = lax.ppermute(base, "expert", flip(size, 2))
    side_b = lax.ppermute(base, "expert", flip(size, 4))
    other_base = lax.ppermute(base, "expert", flip(size, 1))
    up0, up0_done = fetch(w_up, 0, whole, base)
    relay = picked(info, side_b, side_a, up0_done)
    across = lax.ppermute(relay, "expert", mixed)
    other_a = lax.ppermute(side_a, "expert", flip(size, 1))
    other_b = lax.ppermute(side_b, "expert", flip(size, 1))
    gate1, _ = fetch(w_gate, 1, ((0, 1 * tile),), relay)
    other_across = lax.ppermute(across, "expert", flip(size, 1))
    pieces = [base, side_a, side_b, across, other_base, other_a, other_b, other_across]
    held = {(0, 0): gate0, (1, 0): up0, (0, 1): gate1, (1, 1): []}
    mine, theirs = experts_kernel(pieces, info, held, tile, w_gate, w_up, w_down)

    rows = mine.shape[0] // 4
    back = lax.ppermute(theirs, "expert", flip(size, 1))
    quarter = [
        mine[i * rows : (i + 1) * rows] + back[i * rows : (i + 1) * rows].astype(jnp.float32) for i in range(4)
    ]
    got = lax.ppermute(quarter[3].astype(jnp.bfloat16), "expert", mixed).astype(jnp.float32)
    to_a = (quarter[1] + jnp.where(core == 0, 0.0, got)).astype(jnp.bfloat16)
    to_b = (quarter[2] + jnp.where(core == 0, got, 0.0)).astype(jnp.bfloat16)
    from_a = lax.ppermute(to_a, "expert", flip(size, 2))
    from_b = lax.ppermute(to_b, "expert", flip(size, 4))
    total = (quarter[0] + from_a.astype(jnp.float32) + from_b.astype(jnp.float32)).astype(jnp.bfloat16)
    block = rows // depth
    parts = [total[k * block : (k + 1) * block] for k in range(depth)]
    home = [parts[0]] + [lax.ppermute(parts[k], "dp", flip(depth, k)) for k in range(1, depth)]
    return mix_back(info, home, local)


EXPERTS = 8
D = 4096


def slot_table(expert_ids, capacity):
    flat_ids = expert_ids.reshape(-1)
    matches = (flat_ids[:, None] == jnp.arange(EXPERTS, dtype=jnp.int32)[None, :]).astype(jnp.int32)
    before = jnp.cumsum(matches, axis=0) - matches
    rank_in = jnp.sum(before * matches, axis=1)
    limit_of = jnp.sum(matches * capacity[None, :], axis=1)
    slot_of = flat_ids * CAP + rank_in
    chosen = slot_of[None, :] == jnp.arange(EXPERTS * CAP, dtype=jnp.int32)[:, None]
    return chosen & (rank_in < limit_of)[None, :]


def general(tokens, expert_ids, gate_q, capacity, w_gate, w_up, w_down):
    local_experts = w_gate.shape[0]
    groups = lax.axis_size("dp")
    own_table = slot_table(expert_ids, capacity)
    levels = gate_q.astype(jnp.float32)
    mixes = (levels / jnp.sum(levels, axis=1, keepdims=True)).reshape(-1)
    picker = own_table.reshape(EXPERTS * CAP, -1, 2).sum(axis=2).astype(jnp.bfloat16)
    slot_rows = jnp.dot(picker, tokens, preferred_element_type=jnp.float32).astype(jnp.bfloat16)
    slot_rows = slot_rows.reshape(EXPERTS, CAP, D)
    arrived = lax.all_to_all(slot_rows, "dp", split_axis=0, concat_axis=0, tiled=True)
    shard_piece = lax.all_gather(arrived[None], "expert", axis=0, tiled=True)
    amount = shard_piece.shape[0]
    blocks = shard_piece.reshape(amount, groups, local_experts, CAP, D)
    pieces = []
    for member in range(local_experts):
        row_block = blocks[:, :, member].reshape(-1, D)
        gate_val = jnp.dot(row_block, w_gate[member], preferred_element_type=jnp.float32)
        up_value = jnp.dot(row_block, w_up[member], preferred_element_type=jnp.float32)
        result = (jax.nn.silu(gate_val) * up_value).astype(jnp.bfloat16)
        pieces.append(result.reshape(amount, groups, CAP, -1))
    hidden = jnp.stack(pieces, axis=2)
    flat_hidden = hidden.reshape(-1, hidden.shape[-1])
    rows_here = groups * local_experts * CAP
    picked = flat_hidden
    picked = picked.reshape(-1, local_experts, CAP, flat_hidden.shape[-1])
    products = []
    for member in range(local_experts):
        products.append(
            jnp.einsum(
                "mcf,fd->mcd", picked[:, member], w_down[member], preferred_element_type=jnp.float32
            )
        )
    summed = lax.psum_scatter(
        jnp.stack(products, axis=1).reshape(lax.axis_size("expert") * rows_here, -1),
        "expert",
        scatter_dimension=0,
        tiled=True,
    )
    returned = lax.all_to_all(summed, "dp", split_axis=0, concat_axis=0, tiled=True)
    combine = own_table.astype(jnp.float32) * mixes[None, :]
    spread = jnp.einsum("sa,sd->ad", combine, returned, precision=lax.Precision.HIGHEST)
    mixed = spread.reshape(-1, 2, spread.shape[-1]).sum(axis=1)
    return mixed.astype(jnp.bfloat16)


def per_device(tokens, expert_ids, gate_q, capacity, w_gate, w_up, w_down):
    suits = (
        w_gate.shape[0] == 2
        and lax.axis_size("expert") == 8
        and lax.axis_size("dp") == 4
        and tokens.shape[0] == 8
    )
    args = (tokens, expert_ids, gate_q, capacity, w_gate, w_up, w_down)
    if not suits:
        return general(*args)
    return fast(*args)


def solution(mesh):
    in_specs = (
        P(("expert", "dp"), None),
        P(("expert", "dp"), None),
        P(("expert", "dp"), None),
        P(),
        P("dp", None, "expert"),
        P("dp", None, "expert"),
        P("dp", "expert", None),
    )
    out_specs = P(("expert", "dp"), None)
    return jax.shard_map(
        per_device, mesh=mesh, in_specs=in_specs, out_specs=out_specs, check_vma=False
    )
```

```python
import jax
import jax.numpy as jnp
from jax import lax
from jax.experimental import pallas as pl
from jax.experimental.pallas import tpu as pltpu
from jax.sharding import PartitionSpec as P


CAP = 4
LANES = 128
MIB = 1 << 20


VMEM = pl.BlockSpec(memory_space=pltpu.VMEM)
ANY = pl.BlockSpec(memory_space=pl.ANY)
HBM = pl.BlockSpec(memory_space=pltpu.HBM)
SMEM = pl.BlockSpec(memory_space=pltpu.SMEM)


def params(mib):
    return pltpu.CompilerParams(vmem_limit_bytes=int(mib * MIB))


def in_hbm(array):
    return pltpu.with_memory_space_constraint(array, pltpu.HBM)


def iota(shape, dim):
    return lax.broadcasted_iota(jnp.int32, shape, dim)


def pack(tokens, ids, levels, capacity, place):
    rows, width = tokens.shape
    experts = capacity.shape[0]

    def body(place_ref, ids_hbm, level_hbm, cap_hbm, tok_hbm, out_ref, info_ref, ids_ref, level_ref, cap_ref, sems):
        copies = [
            pltpu.make_async_copy(src, dst, sems.at[i])
            for i, (src, dst) in enumerate(
                (
                    (ids_hbm, ids_ref),
                    (level_hbm, level_ref),
                    (cap_hbm, cap_ref),
                    (tok_hbm, out_ref.at[:, pl.ds(0, width)]),
                )
            )
        ]
        for copy in copies:
            copy.start()
        for copy in copies:
            copy.wait()
        eye = iota((rows, rows), 0) == iota((rows, rows), 1)
        lower = (iota((rows, rows), 1) < iota((rows, rows), 0)).astype(jnp.float32)
        expert = iota((rows, experts), 1).astype(jnp.float32)
        limits = cap_ref[...].astype(jnp.float32)

        def column(ref, k):
            return jnp.sum(jnp.where(eye, ref[k : k + 1, :].astype(jnp.float32), 0.0), axis=1, keepdims=True)

        named = [column(ids_ref, k) for k in range(2)]
        hot = [(expert == col).astype(jnp.float32) for col in named]
        before = jnp.dot(lower, hot[0] + hot[1], preferred_element_type=jnp.float32)
        level = [column(level_ref, k) for k in range(2)]
        total = level[0] + level[1]
        lane = iota((rows, LANES), 1)
        slots = jnp.full((rows, LANES), -1.0, jnp.float32)
        info = slots
        for k in range(2):
            rank = jnp.sum(hot[k] * before, axis=1, keepdims=True)
            limit = jnp.sum(hot[k] * limits, axis=1, keepdims=True)
            slot = jnp.where(rank < limit, named[k] * CAP + rank, -1.0)
            slots = jnp.where(lane == k, slot, slots)
            info = jnp.where(lane == k, slot, jnp.where(lane == 2 + k, level[k] / total, info))
        for i in range(2):
            info = jnp.where(lane == 4 + i, place_ref[i].astype(jnp.float32), info)
        out_ref[:, width:] = slots.astype(jnp.bfloat16)
        info_ref[...] = info

    return pl.pallas_call(
        body,
        in_specs=[SMEM] + [HBM] * 4,
        out_specs=[VMEM] * 2,
        out_shape=[
            jax.ShapeDtypeStruct((rows, width + LANES), jnp.bfloat16),
            jax.ShapeDtypeStruct((rows, LANES), jnp.float32),
        ],
        scratch_shapes=[
            pltpu.VMEM(ids.shape, jnp.int32),
            pltpu.VMEM(levels.shape, jnp.int32),
            pltpu.VMEM((1, experts), jnp.int32),
            pltpu.SemaphoreType.DMA((4,)),
        ],
        compiler_params=params(0.5),
        name="pack",
    )(place, *map(in_hbm, (ids, levels, capacity.reshape(1, experts), tokens)))


def mix_back(info, pieces, local):
    rows = info.shape[0]
    width = pieces[0].shape[1]
    span = local * CAP

    def body(info_ref, *refs):
        *ins, out_ref = refs
        here = info_ref[:, 4:5].astype(jnp.int32)
        row = iota((rows, span), 1)
        weights = []
        for q in range(len(ins)):
            group = here ^ q
            weight = jnp.zeros((rows, span), jnp.float32)
            for k in range(2):
                slot = info_ref[:, k : k + 1].astype(jnp.int32) - group * span
                if q % 2:
                    slot = jnp.where((slot < 0) | (slot >= span), -1, slot ^ CAP)
                weight = weight + jnp.where(row == slot, info_ref[:, 2 + k : 3 + k], 0.0)
            weights.append(weight)
        weight = jnp.concatenate(weights, axis=1)
        terms = []
        for _ in range(3):
            terms.append(weight.astype(jnp.bfloat16).astype(jnp.float32))
            weight = weight - terms[-1]
        terms = jnp.concatenate(terms + [jnp.zeros_like(weight)], axis=0).astype(jnp.bfloat16)
        blocks = jnp.concatenate([ref[...] for ref in ins], axis=0)
        sums = jnp.dot(terms, blocks, preferred_element_type=jnp.float32)
        total = sums[:rows] + sums[rows : 2 * rows] + sums[2 * rows : 3 * rows]
        out_ref[...] = total.astype(jnp.bfloat16)

    return pl.pallas_call(
        body,
        in_specs=[VMEM] * (1 + len(pieces)),
        out_specs=VMEM,
        out_shape=jax.ShapeDtypeStruct((rows, width), jnp.bfloat16),
        compiler_params=params(8),
        name="mix_back",
    )(info, *pieces)


def fetch(weights, member, splits, after):
    depth = weights.shape[1]
    parts = 4
    step = depth // parts
    count = len(splits)

    def body(w_ref, after_ref, *refs):
        outs, done_ref, sems = refs[:count], refs[count], refs[count + 1]
        copies = []
        for j, (first, width) in enumerate(splits):
            for i in range(parts):
                part = pl.ds(i * step, step)
                copies.append(
                    pltpu.make_async_copy(
                        w_ref.at[member, part, pl.ds(first, width)], outs[j].at[part], sems.at[j * parts + i]
                    )
                )
        for copy in copies:
            copy.start()
        for copy in copies:
            copy.wait()
        done_ref[...] = jnp.zeros_like(done_ref)

    *blocks, done = pl.pallas_call(
        body,
        in_specs=[HBM, ANY],
        out_specs=[VMEM] * (count + 1),
        out_shape=[pltpu.VMEM((depth, width), jnp.bfloat16) for _, width in splits]
        + [jax.ShapeDtypeStruct((8, LANES), jnp.float32)],
        scratch_shapes=[pltpu.SemaphoreType.DMA((parts * count,))],
        compiler_params=params(0.25),
    )(in_hbm(weights), after)
    return blocks, done


def joined(pieces, after):
    rows, width = pieces[0].shape
    count = len(pieces)

    def body(*refs):
        out_ref = refs[-1]
        for i in range(count):
            out_ref[i * rows : (i + 1) * rows, :] = refs[i][...]

    return pl.pallas_call(
        body,
        in_specs=[VMEM] * count + [ANY],
        out_specs=VMEM,
        out_shape=jax.ShapeDtypeStruct((count * rows, width), pieces[0].dtype),
        compiler_params=params(1),
    )(*pieces, after)


def picked(info, first, second, after):
    rows = first.shape[0]

    def body(info_ref, first_ref, second_ref, after_ref, out_ref):
        even = jnp.broadcast_to(info_ref[0:1, 5:6], (rows, 1)) == 0.0

        out_ref[...] = jnp.where(even, first_ref[...], second_ref[...])

    return pl.pallas_call(
        body,
        in_specs=[VMEM, VMEM, VMEM, ANY],
        out_specs=VMEM,
        out_shape=jax.ShapeDtypeStruct(first.shape, first.dtype),
        compiler_params=params(1),
    )(info, first, second, after)


def experts_kernel(pieces, info, held, tile, w_gate, w_up, w_down):
    local, width, units = w_gate.shape
    groups = len(pieces)
    piece_rows = pieces[0].shape[0]
    tokens = groups * piece_rows
    slots = tokens // 8 * CAP
    steps = units // tile
    down_steps = width // tile
    ring = 5
    batch = 2
    half = groups // 2 * piece_rows
    order = [(matrix, member) for member in range(local) for matrix in range(2)]
    given = [block for key in order for block in held[key]]

    def body(*refs):
        piece_refs = refs[:groups]
        info_ref = refs[groups]
        given_refs = list(refs[groups + 1 : groups + 1 + len(given)])
        wg, wu, wd, mine, theirs, toks, rows, hid, buf, sems = refs[groups + 1 + len(given) :]

        tiles, stream = {}, []
        for key in order:
            at = 0
            for block in held[key]:
                ref = given_refs.pop(0)
                for n in range(block.shape[1] // tile):
                    tiles[key, at] = (ref, n)
                    at += 1
        for member in range(local):
            for n in range(steps):
                for matrix in range(2):
                    if ((matrix, member), n) not in tiles:
                        tiles[(matrix, member), n] = len(stream)
                        stream.append(((wg, wu)[matrix], member, n))

        downs = len(stream)
        jobs = downs + down_steps

        def copies(i):
            at = i % ring
            if i < downs:
                w, member, n = stream[i]
                pairs = [(w.at[member, :, pl.ds(n * tile, tile)], buf.at[at])]
            else:
                cols = pl.ds((i - downs) * tile, tile)
                pairs = [(wd.at[m, :, cols], buf.at[at, pl.ds(m * units, units)]) for m in range(local)]
            return [pltpu.make_async_copy(*pair, sems.at[at, j]) for j, pair in enumerate(pairs)]

        def start(i):
            if i < jobs:
                for copy in copies(i):
                    copy.start()

        def wait(i):
            for copy in copies(i):
                copy.wait()

        for i in range(ring):
            start(i)

        first = info_ref[0:1, 4:5].astype(jnp.int32) * (local * CAP)
        token_block = iota((tokens, slots), 0) // 8
        slot = iota((tokens, slots), 1)
        slot_block = slot // CAP
        slot_rank = slot % CAP
        pick = [jnp.zeros((tokens, slots), jnp.bool_) for _ in range(local)]
        for g in range(groups):
            toks[g * piece_rows : (g + 1) * piece_rows, :] = piece_refs[g][:, :width]
        for k in range(2):
            code = jnp.concatenate(
                [ref[:, width : width + LANES].astype(jnp.float32)[:, k : k + 1] for ref in piece_refs], axis=0
            ).astype(jnp.int32)
            for m in range(local):
                hit = (code - first == slot_rank + m * CAP) & (token_block == (slot_block ^ m))
                pick[m] = pick[m] | hit
        pickers = [p.astype(jnp.float32).T.astype(jnp.bfloat16) for p in pick]

        def place(n, carry):
            cols = pl.ds(pl.multiple_of(n * tile, tile), tile)
            for m in range(local):
                rows[m, :, cols] = jnp.dot(pickers[m], toks[:, cols], preferred_element_type=jnp.float32).astype(
                    jnp.bfloat16
                )
            return carry

        lax.fori_loop(0, width // tile, place, 0)

        def product(matrix, m, n):
            spot = tiles[(matrix, m), n]
            if isinstance(spot, tuple):
                ref, at = spot
                block = ref[:, at * tile : (at + 1) * tile]
            else:
                block = buf[spot % ring, :width, :]
            return jnp.dot(rows[m], block, preferred_element_type=jnp.float32)

        def streamed(m, n):
            return [spot for matrix in range(2) if not isinstance(spot := tiles[(matrix, m), n], tuple)]

        waiting, ready = [], []
        for m in range(local):
            for n in range(steps):
                spots = streamed(m, n)
                if not spots:
                    ready.append(([(m, n)], []))
                elif waiting and len(waiting[-1][1]) + len(spots) <= batch:
                    waiting[-1][0].append((m, n))
                    waiting[-1][1].extend(spots)
                else:
                    waiting.append(([(m, n)], spots))
        turns = []
        while waiting or ready:
            turns += [queue.pop(0) for queue in (waiting, ready) if queue]
        for group, spots in turns:
            for spot in spots:
                wait(spot)
            for m, n in group:
                gate = product(0, m, n)
                up = product(1, m, n)
                act = gate * (1.0 / (1.0 + jnp.exp(-gate))) * up
                hid[m, :, n * tile : (n + 1) * tile] = act.astype(jnp.bfloat16)
            for spot in spots:
                start(spot + ring)

        low = iota((8, tile), 0) < CAP
        for n in range(down_steps):
            cols = slice(n * tile, (n + 1) * tile)
            if n % batch == 0:
                for i in range(n, min(n + batch, down_steps)):
                    wait(downs + i)
            slot_at = (downs + n) % ring
            outs = [
                jnp.dot(hid[m], buf[slot_at, m * units : (m + 1) * units, :], preferred_element_type=jnp.float32)
                for m in range(local)
            ]
            start(downs + n + ring)
            for j in range(slots // 8):
                a, b = (out[j * 8 : (j + 1) * 8] for out in outs)
                pair = jnp.concatenate([jnp.where(low, a, b), jnp.where(low, b, a)], axis=0)
                at = j * 16
                if at < half:
                    mine[at : at + 16, cols] = pair
                else:
                    theirs[at - half : at - half + 16, cols] = pair.astype(jnp.bfloat16)

    bf16 = jnp.bfloat16
    return pl.pallas_call(
        body,
        in_specs=[VMEM] * (groups + 1 + len(given)) + [HBM] * 3,
        out_specs=[VMEM] * 2,
        out_shape=[
            jax.ShapeDtypeStruct((half, width), jnp.float32),
            jax.ShapeDtypeStruct((half, width), bf16),
        ],
        scratch_shapes=[
            pltpu.VMEM((tokens, width), bf16),
            pltpu.VMEM((local, slots, width), bf16),
            pltpu.VMEM((local, slots, units), bf16),
            pltpu.VMEM((ring, max(width, local * units), tile), bf16),
            pltpu.SemaphoreType.DMA((ring, local)),
        ],
        compiler_params=params(16.2),
        name="experts",
    )(*pieces, info, *given, *map(in_hbm, (w_gate, w_up, w_down)))


def flip(size, bits):
    return [(i, i ^ bits) for i in range(size)]


def fast(tokens, expert_ids, gate_q, capacity, w_gate, w_up, w_down):
    size = lax.axis_size("expert")
    depth = lax.axis_size("dp")
    local, _, units = w_gate.shape
    core = jnp.bitwise_and(lax.axis_index("expert"), 1)
    place = jnp.stack([lax.axis_index("dp"), core]).astype(jnp.int32)
    mixed = [(i, i ^ (2 if i % 2 == 0 else 4)) for i in range(size)]

    packed, info = pack(tokens, expert_ids.T, gate_q.T, capacity, place)
    along = [packed] + [lax.ppermute(packed, "dp", flip(depth, k)) for k in range(1, depth)]
    tile = 256
    some, rest = 2 * tile, units - 4 * tile
    whole = ((0, some), (some, some), (2 * some, rest))
    gate0, gate0_done = fetch(w_gate, 0, whole, packed)
    base = joined(along, gate0_done)
    side_a = lax.ppermute(base, "expert", flip(size, 2))
    side_b = lax.ppermute(base, "expert", flip(size, 4))
    other_base = lax.ppermute(base, "expert", flip(size, 1))
    up0, up0_done = fetch(w_up, 0, whole, base)
    relay = picked(info, side_b, side_a, up0_done)
    across = lax.ppermute(relay, "expert", mixed)
    other_a = lax.ppermute(side_a, "expert", flip(size, 1))
    other_b = lax.ppermute(side_b, "expert", flip(size, 1))
    gate1, _ = fetch(w_gate, 1, ((0, 2 * tile),), relay)
    other_across = lax.ppermute(across, "expert", flip(size, 1))
    pieces = [base, side_a, side_b, across, other_base, other_a, other_b, other_across]
    held = {(0, 0): gate0, (1, 0): up0, (0, 1): gate1, (1, 1): []}
    mine, theirs = experts_kernel(pieces, info, held, tile, w_gate, w_up, w_down)

    rows = mine.shape[0] // 4
    back = lax.ppermute(theirs, "expert", flip(size, 1))
    quarter = [
        mine[i * rows : (i + 1) * rows] + back[i * rows : (i + 1) * rows].astype(jnp.float32) for i in range(4)
    ]
    got = lax.ppermute(quarter[3].astype(jnp.bfloat16), "expert", mixed).astype(jnp.float32)
    to_a = (quarter[1] + jnp.where(core == 0, 0.0, got)).astype(jnp.bfloat16)
    to_b = (quarter[2] + jnp.where(core == 0, got, 0.0)).astype(jnp.bfloat16)
    from_a = lax.ppermute(to_a, "expert", flip(size, 2))
    from_b = lax.ppermute(to_b, "expert", flip(size, 4))
    total = (quarter[0] + from_a.astype(jnp.float32) + from_b.astype(jnp.float32)).astype(jnp.bfloat16)
    block = rows // depth
    parts = [total[k * block : (k + 1) * block] for k in range(depth)]
    home = [parts[0]] + [lax.ppermute(parts[k], "dp", flip(depth, k)) for k in range(1, depth)]
    return mix_back(info, home, local)


EXPERTS = 8
D = 4096


def slot_table(expert_ids, capacity):
    flat_ids = expert_ids.reshape(-1)
    matches = (flat_ids[:, None] == jnp.arange(EXPERTS, dtype=jnp.int32)[None, :]).astype(jnp.int32)
    before = jnp.cumsum(matches, axis=0) - matches
    rank_in = jnp.sum(before * matches, axis=1)
    limit_of = jnp.sum(matches * capacity[None, :], axis=1)
    slot_of = flat_ids * CAP + rank_in
    chosen = slot_of[None, :] == jnp.arange(EXPERTS * CAP, dtype=jnp.int32)[:, None]
    return chosen & (rank_in < limit_of)[None, :]


def general(tokens, expert_ids, gate_q, capacity, w_gate, w_up, w_down):
    local_experts = w_gate.shape[0]
    groups = lax.axis_size("dp")
    own_table = slot_table(expert_ids, capacity)
    levels = gate_q.astype(jnp.float32)
    mixes = (levels / jnp.sum(levels, axis=1, keepdims=True)).reshape(-1)
    picker = own_table.reshape(EXPERTS * CAP, -1, 2).sum(axis=2).astype(jnp.bfloat16)
    slot_rows = jnp.dot(picker, tokens, preferred_element_type=jnp.float32).astype(jnp.bfloat16)
    slot_rows = slot_rows.reshape(EXPERTS, CAP, D)
    arrived = lax.all_to_all(slot_rows, "dp", split_axis=0, concat_axis=0, tiled=True)
    shard_piece = lax.all_gather(arrived[None], "expert", axis=0, tiled=True)
    amount = shard_piece.shape[0]
    blocks = shard_piece.reshape(amount, groups, local_experts, CAP, D)
    pieces = []
    for member in range(local_experts):
        row_block = blocks[:, :, member].reshape(-1, D)
        gate_val = jnp.dot(row_block, w_gate[member], preferred_element_type=jnp.float32)
        up_value = jnp.dot(row_block, w_up[member], preferred_element_type=jnp.float32)
        result = (jax.nn.silu(gate_val) * up_value).astype(jnp.bfloat16)
        pieces.append(result.reshape(amount, groups, CAP, -1))
    hidden = jnp.stack(pieces, axis=2)
    flat_hidden = hidden.reshape(-1, hidden.shape[-1])
    rows_here = groups * local_experts * CAP
    picked = flat_hidden
    picked = picked.reshape(-1, local_experts, CAP, flat_hidden.shape[-1])
    products = []
    for member in range(local_experts):
        products.append(
            jnp.einsum(
                "mcf,fd->mcd", picked[:, member], w_down[member], preferred_element_type=jnp.float32
            )
        )
    summed = lax.psum_scatter(
        jnp.stack(products, axis=1).reshape(lax.axis_size("expert") * rows_here, -1),
        "expert",
        scatter_dimension=0,
        tiled=True,
    )
    returned = lax.all_to_all(summed, "dp", split_axis=0, concat_axis=0, tiled=True)
    combine = own_table.astype(jnp.float32) * mixes[None, :]
    spread = jnp.einsum("sa,sd->ad", combine, returned, precision=lax.Precision.HIGHEST)
    mixed = spread.reshape(-1, 2, spread.shape[-1]).sum(axis=1)
    return mixed.astype(jnp.bfloat16)


def per_device(tokens, expert_ids, gate_q, capacity, w_gate, w_up, w_down):
    suits = (
        w_gate.shape[0] == 2
        and lax.axis_size("expert") == 8
        and lax.axis_size("dp") == 4
        and tokens.shape[0] == 8
    )
    args = (tokens, expert_ids, gate_q, capacity, w_gate, w_up, w_down)
    if not suits:
        return general(*args)
    return fast(*args)


def solution(mesh):
    in_specs = (
        P(("expert", "dp"), None),
        P(("expert", "dp"), None),
        P(("expert", "dp"), None),
        P(),
        P("dp", None, "expert"),
        P("dp", None, "expert"),
        P("dp", "expert", None),
    )
    out_specs = P(("expert", "dp"), None)
    return jax.shard_map(
        per_device, mesh=mesh, in_specs=in_specs, out_specs=out_specs, check_vma=False
    )
```
